32 devices in a mesh: node: 8 (over y, x, core), local: 4 (over z).
Axes of the slice: x: 2, y: 2, z: 4, core: 2. Of those that a mesh axis runs over, the one named last changes fastest.
Arguments:
- tokens: bfloat16 [32, 7168], P(('node', 'local')), may hold values from -6 to 6
- w_gate: bfloat16 [16, 1024, 7168], P('node', 'local'), may hold values from -0.0625 to 0.0625
- w_up: bfloat16 [16, 1024, 7168], P('node', 'local'), may hold values from -0.0625 to 0.0625
- w_down: bfloat16 [16, 1024, 7168], P('node', 'local'), may hold values from -0.1875 to 0.1875
- expert_ids: int32 [32, 8], P(('node', 'local')), may hold values from 0 to 15, all different within a row
- gate_ints: int32 [32, 8], P(('node', 'local')), may hold values from 1 to 8
Outputs:
- mixed: bfloat16 [32, 7168], P(('node', 'local'))
The draws below stay inside these ranges and needn't reach their ends.
Inputs may be any that keep to these rules, and one draw needn't show every extreme that they name: `expert_ids`: each row names 8 different experts.
All inputs are finite; a program needn't handle non-finite values.
Results may differ from the reference program's by a relative error of at most 0.025.
Values may be sent and summed in bfloat16 or wider, within the bound.
A program may use at most 64 MiB of HBM per device.

```python
import jax
import jax.numpy as jnp
from jax import lax

D = 7168
FF = 1024
TOP = 8
EXP_NODE = 2
CAP = 8
TOK_DEV = 1
EXPERTS = 16
TOKENS = 32
FFL = 256
N_NODE = 8
N_LOCAL = 4


def touch_ends(values, own_key, smallest, high):
    place = [jax.random.randint(jax.random.fold_in(own_key, axis), (), 0, length) for axis, length in enumerate(values.shape)]
    widest = values.shape.index(max(values.shape))
    neighbour = place[:widest] + [(place[widest] + 1) % values.shape[widest]] + place[widest + 1:]
    return values.at[tuple(place)].set(smallest).at[tuple(neighbour)].set(high)


def block_levels(rng, extent, pieces, least, top_value):
    loudness = 1.0
    for axis_at, parts in pieces:
        steps = jax.random.uniform(jax.random.fold_in(jax.random.fold_in(rng, 6), axis_at), (parts,), jnp.float32, least / len(pieces), top_value / len(pieces))
        loudness = loudness * jnp.repeat(jnp.exp(steps), extent[axis_at] // parts).reshape((-1,) + (1,) * (len(extent) - 1 - axis_at))
    return loudness


def distinct(stream_key, rows, count, top, lift):
    ranking = jax.random.permutation(jax.random.fold_in(stream_key, 1), count)
    boost = ranking
    for power in range(3):
        boost = boost * boost // count
    boost = boost * lift // count
    lots = jax.random.randint(jax.random.fold_in(stream_key, 2), (rows, count), 0, 4096) + boost
    fixed_rows = jax.random.permutation(jax.random.fold_in(stream_key, 3), rows)[jnp.arange(count) % rows]
    lots = jnp.where(jnp.arange(rows)[:, None] == fixed_rows[None, :], 1 << 14, lots)
    score = lots * count + jnp.arange(count)
    return lax.top_k(score.astype(jnp.int32), top)[1].astype(jnp.int32)


def normal_values(stream_key, shape, width, limit, shards=(), held_as=jnp.bfloat16):
    loudness = block_levels(stream_key, shape, shards, -0.22, 0.18) if shards else 1.0
    entries = jax.random.normal(stream_key, shape, jnp.float32) * width * loudness
    return jnp.minimum(jnp.maximum(entries, -limit), limit).astype(held_as)


def setup_inputs(seed: int = 0) -> dict:
    splits = jax.random.split(jax.random.key(seed), 7)
    tokens = normal_values(splits[0], (TOKENS, D), 1.0, 6.0, ((0, 32),))
    w_gate = normal_values(splits[1], (EXPERTS, FF, D), D ** -0.5, 0.0625, ((0, 8), (1, 4)))
    w_up = normal_values(splits[2], (EXPERTS, FF, D), D ** -0.5, 0.0625, ((0, 8), (1, 4)))
    w_down = normal_values(splits[3], (EXPERTS, FF, D), FF ** -0.5, 0.1875, ((0, 8), (1, 4)))
    expert_ids = distinct(splits[4], TOKENS, EXPERTS, TOP, 8192)
    gate_ints = touch_ends(jax.random.randint(splits[5], (TOKENS, TOP), 1, 9), jax.random.fold_in(splits[5], 1), 1, 8).astype(jnp.int32)
    return dict(tokens=tokens, w_gate=w_gate, w_up=w_up, w_down=w_down, expert_ids=expert_ids, gate_ints=gate_ints)


def reference(tokens, w_gate, w_up, w_down, expert_ids, gate_ints):
    slot_count = N_NODE * TOK_DEV
    by_column = tokens.reshape(N_NODE, N_LOCAL, TOK_DEV, D).transpose(1, 0, 2, 3).reshape(N_LOCAL, slot_count, D)
    ids_column = expert_ids.reshape(N_NODE, N_LOCAL, TOK_DEV, TOP).transpose(1, 0, 2, 3).reshape(N_LOCAL, slot_count, TOP)
    gates_column = gate_ints.reshape(N_NODE, N_LOCAL, TOK_DEV, TOP).transpose(1, 0, 2, 3).reshape(N_LOCAL, slot_count, TOP)
    slot_iota = jnp.arange(CAP, dtype=jnp.int32)
    row_count = N_LOCAL * CAP
    rows_f32 = by_column.astype(jnp.float32)

    def per_node(total, group):
        wanted = group * EXP_NODE + jnp.arange(EXP_NODE, dtype=jnp.int32)
        matched = ids_column[..., None] == wanted
        gate_sums = jnp.sum(jnp.where(matched, gates_column[..., None], 0), axis=2).astype(jnp.int32)
        is_hit = (jnp.sum(gate_sums, axis=-1) > 0).astype(jnp.int32)
        slot_rank = jnp.cumsum(is_hit, axis=1).astype(jnp.int32) - is_hit
        keep_flag = (is_hit > 0) & (slot_rank < CAP)
        picker = (keep_flag[:, None, :] & (slot_rank[:, None, :] == slot_iota[None, :, None])).astype(jnp.float32)
        packed = jnp.einsum('lcs,lsd->lcd', picker, rows_f32).astype(jnp.bfloat16).reshape(row_count, D)
        packed_gates = jnp.einsum('lcs,lse->lce', picker, gate_sums.astype(jnp.float32)).reshape(row_count, EXP_NODE) / 8.0
        first = (group * EXP_NODE).astype(jnp.int32)
        gate_w = lax.dynamic_slice_in_dim(w_gate, first, EXP_NODE, 0).astype(jnp.float32)
        up_w = lax.dynamic_slice_in_dim(w_up, first, EXP_NODE, 0).astype(jnp.float32)
        down_w = lax.dynamic_slice_in_dim(w_down, first, EXP_NODE, 0)
        packed_f32 = packed.astype(jnp.float32)
        gate_act = jnp.einsum('rd,efd->ref', packed_f32, gate_w)
        up_act = jnp.einsum('rd,efd->ref', packed_f32, up_w)
        hidden = (jax.nn.silu(gate_act) * up_act * packed_gates[:, :, None]).astype(jnp.bfloat16)
        hidden_blocks = hidden.reshape(row_count, EXP_NODE, N_LOCAL, FFL).transpose(2, 0, 1, 3).reshape(N_LOCAL, row_count, EXP_NODE * FFL)
        down_blocks = down_w.reshape(EXP_NODE, N_LOCAL, FFL, D).transpose(1, 0, 2, 3).reshape(N_LOCAL, EXP_NODE * FFL, D)

        def add_block(acc, block_pair):
            part = jnp.dot(block_pair[0], block_pair[1], preferred_element_type=jnp.float32)
            rounded = lax.optimization_barrier(part.astype(jnp.bfloat16))
            return acc + rounded.astype(jnp.float32), None

        summed, _ = lax.scan(add_block, jnp.zeros((row_count, D), jnp.float32), (hidden_blocks, down_blocks))
        group_out = summed.astype(jnp.bfloat16).reshape(N_LOCAL, CAP, D).astype(jnp.float32)
        placed = jnp.einsum('lcs,lcd->lsd', picker, group_out)
        return total + placed, None

    start = jnp.zeros((N_LOCAL, slot_count, D), jnp.float32)
    total, _ = lax.scan(per_node, start, jnp.arange(N_NODE, dtype=jnp.int32))
    mixed = total.astype(jnp.bfloat16).reshape(N_LOCAL, N_NODE, TOK_DEV, D).transpose(1, 0, 2, 3).reshape(N_NODE * N_LOCAL * TOK_DEV, D)
    return mixed
```

```python
import functools

import jax
import jax.numpy as jnp
from jax import lax
from jax.experimental import pallas as pl
from jax.experimental.pallas import tpu as pltpu
from jax.sharding import PartitionSpec as P

CAP = 8


def on_device(tokens, w_gate, w_up, w_down, expert_ids, gate_ints):
    node_count = lax.axis_size("node")
    tok_dev = tokens.shape[0]
    model_width = tokens.shape[1]
    exp_node = w_gate.shape[0]
    slot_count = node_count * tok_dev
    wanted = jnp.arange(node_count * exp_node, dtype=jnp.int32).reshape(node_count, exp_node)
    matched = expert_ids[None, :, :, None] == wanted[:, None, None, :]
    gate_sums = jnp.sum(jnp.where(matched, gate_ints[None, :, :, None], 0), axis=2)
    is_hit = jnp.sum(gate_sums, axis=-1) > 0
    outgoing = jnp.where(is_hit[:, :, None], tokens[None, :, :], jnp.zeros_like(tokens)[None, :, :])
    rows_in, gates_in = (
        lax.all_to_all(outgoing, "node", split_axis=0, concat_axis=0, tiled=True),
        lax.all_to_all(
            gate_sums.astype(jnp.bfloat16), "node", split_axis=0, concat_axis=0, tiled=True
        ),
    )
    flat_rows = rows_in.reshape(slot_count, model_width)
    flat_gates = gates_in.reshape(slot_count, exp_node)
    present = (jnp.sum(flat_gates.astype(jnp.float32), axis=-1) > 0).astype(jnp.int32)
    slot_rank = jnp.cumsum(present) - present
    picker = (
        (present[None, :] > 0) & (slot_rank[None, :] == jnp.arange(CAP, dtype=jnp.int32)[:, None])
    ).astype(jnp.bfloat16)
    packed = jnp.dot(picker, flat_rows, preferred_element_type=jnp.float32).astype(jnp.bfloat16)
    packed_gates = jnp.dot(picker, flat_gates, preferred_element_type=jnp.float32).astype(
        jnp.bfloat16
    )
    all_rows, all_gates = (
        lax.all_gather(packed, "local", axis=0, tiled=True),
        lax.all_gather(packed_gates, "local", axis=0, tiled=True),
    )
    gate_act = jnp.einsum("rd,efd->ref", all_rows, w_gate, preferred_element_type=jnp.float32)
    up_act = jnp.einsum("rd,efd->ref", all_rows, w_up, preferred_element_type=jnp.float32)
    scales = all_gates.astype(jnp.float32) / 8.0
    hidden = (jax.nn.silu(gate_act) * up_act * scales[:, :, None]).astype(jnp.bfloat16)
    hidden = hidden.reshape(hidden.shape[0], -1)
    down_flat = w_down.reshape(-1, model_width)
    partial_value = jnp.dot(hidden, down_flat, preferred_element_type=jnp.float32)
    summed = lax.psum_scatter(
        partial_value.astype(jnp.bfloat16), "local", scatter_dimension=0, tiled=True
    )
    unpacked = jnp.dot(picker.T, summed, preferred_element_type=jnp.float32).astype(jnp.bfloat16)
    unpacked = unpacked.reshape(node_count, tok_dev, model_width)
    returned = lax.all_to_all(unpacked, "node", split_axis=0, concat_axis=0, tiled=True)
    return jnp.sum(returned.astype(jnp.float32), axis=0).astype(jnp.bfloat16)


LANES = 128
BF16 = jnp.bfloat16
F32 = jnp.float32


def flip(value, mask):
    bit = 1
    out = value
    while bit <= mask:
        if mask & bit:
            out = out + bit - 2 * bit * ((value // bit) % 2)
        bit *= 2
    return out


def kernel(
    nodes, locals_, tok_ref, ids_ref, gate_ints_ref, wg_hbm, wu_hbm, wd_hbm, out_ref,
    wg, wu, wd, xbuf, xf, xs, acc, ps, pr, pf, qf, qs, r2, ss, r3, of,
    w_sem, x_send, x_recv, p_send, p_recv, q_send, q_recv, s_send, s_recv,
):
    chips = nodes // 2
    rows = nodes * locals_
    half = rows // 2
    width = tok_ref.shape[1]
    pieces = width // LANES
    pitch = xbuf.shape[1]
    experts, ffl = wg.shape[0], wg.shape[1]
    me_n = lax.axis_index("node")
    me_l = lax.axis_index("local")

    def peer(offset):
        core, rest = offset // half, offset % half
        chip, loc = rest // locals_, rest % locals_
        return (flip(me_n, chip * 2 + core), flip(me_l, loc))

    z_offsets = list(range(1, locals_))
    c_offsets = [c * locals_ for c in range(1, chips)]
    partner = half
    barrier = pltpu.get_barrier_semaphore()
    greeted = z_offsets + c_offsets + [partner]
    for offset in greeted:
        pl.semaphore_signal(
            barrier, inc=1, device_id=peer(offset), device_id_type=pl.DeviceIdType.MESH
        )

    loads = []
    for which, (source, dest) in enumerate(((wg_hbm, wg), (wu_hbm, wu), (wd_hbm, wd))):
        for e in range(experts):
            copy = pltpu.make_async_copy(source.at[e], dest.at[e], w_sem.at[which, e])
            copy.start()
            loads.append(copy)

    xf[0:pitch, :] = jnp.zeros((pitch, LANES), F32)
    for k in range(pieces):
        xf[k : k + 1, :] = tok_ref[:, k * LANES : (k + 1) * LANES].astype(F32)
    top = ids_ref.shape[1]
    xf[pieces : pieces + 1, 0:top] = ids_ref[...].astype(F32)
    xf[pieces + 1 : pieces + 2, 0:top] = gate_ints_ref[...].astype(F32)
    xbuf[0] = xf[0:pitch, :].astype(BF16)

    pl.semaphore_wait(barrier, len(greeted))

    waits = []

    def send(row, offset, slot):
        copy = pltpu.make_async_remote_copy(
            src_ref=xbuf.at[row],
            dst_ref=xbuf.at[row ^ offset],
            send_sem=x_send.at[slot, row],
            recv_sem=x_recv.at[row ^ offset],
            device_id=peer(offset),
            device_id_type=pl.DeviceIdType.MESH,
        )
        copy.start()
        waits.append(copy)

    def arrive(row):
        pltpu.make_async_remote_copy(
            src_ref=xbuf.at[row],
            dst_ref=xbuf.at[row],
            send_sem=x_send.at[0, row],
            recv_sem=x_recv.at[row],
            device_id=peer(partner),
            device_id_type=pl.DeviceIdType.MESH,
        ).wait_recv()

    def widen(row):
        xf[row * pitch : (row + 1) * pitch, :] = xbuf[row].astype(F32)

    for number, offset in enumerate(z_offsets):
        send(0, offset, 1 + chips + number)
    for number, offset in enumerate(c_offsets):
        send(0, offset, 1 + number)
    send(0, partner, 0)
    for row in z_offsets:
        arrive(row)
        for number, offset in enumerate(c_offsets):
            send(row, offset, 1 + number)
        send(row, partner, 0)
        widen(row)
    for loc in range(locals_):
        for offset in c_offsets:
            row = offset + loc
            arrive(row)
            send(row, partner, 0)
            widen(row)
    for loc in range(locals_):
        for offset in [0] + c_offsets:
            arrive(half + offset + loc)
            widen(half + offset + loc)

    for k in range(pieces):
        xs[:, k * LANES : (k + 1) * LANES] = xf[pl.ds(k, rows, stride=pitch), :].astype(BF16)
    ids = xf[pl.ds(pieces, rows, stride=pitch), :]
    gates = xf[pl.ds(pieces + 1, rows, stride=pitch), :]
    scales = []
    for e in range(experts):
        named = (me_n * experts + e).astype(F32)
        picked = jnp.where(ids == named, gates, 0.0)
        scales.append(jnp.sum(picked, axis=1, keepdims=True) / 8.0)

    for copy in loads[: 2 * experts]:
        copy.wait()
    chunk = 1024 if width % 1024 == 0 else width
    acc[...] = jnp.zeros_like(acc)

    def depth_step(step, carry):
        at = pl.ds(pl.multiple_of(step * chunk, chunk), chunk)
        x = xs[:, at]
        for which, weights in enumerate((wg, wu)):
            for e in range(experts):
                acc[which, e] += lax.dot_general(
                    weights[e, :, at], x, (((1,), (1,)), ((), ())), preferred_element_type=F32
                )
        return carry

    lax.fori_loop(0, width // chunk, depth_step, 0)
    hidden = []
    for e in range(experts):
        g = acc[0, e].T
        u = acc[1, e].T
        hidden.append((g / (1.0 + jnp.exp(-g)) * u * scales[e]).astype(BF16))

    for copy in loads[2 * experts :]:
        copy.wait()
    sends = []
    steps = width // chunk

    def partner_copy(step):
        at = pl.ds(step * chunk, chunk)
        return pltpu.make_async_remote_copy(
            src_ref=ps.at[:, at],
            dst_ref=pr.at[:, at],
            send_sem=p_send.at[step],
            recv_sem=p_recv.at[step],
            device_id=peer(partner),
            device_id_type=pl.DeviceIdType.MESH,
        )

    for step in range(steps):
        at = slice(step * chunk, (step + 1) * chunk)
        part = jnp.dot(hidden[0], wd[0, :, at], preferred_element_type=F32)
        for e in range(1, experts):
            part += jnp.dot(hidden[e], wd[e, :, at], preferred_element_type=F32)
        ps[:, at] = part[half:].astype(BF16)
        pf[:, at] = part[:half]
        sends.append(partner_copy(step))
        if step:
            sends[step - 1].start()
    sends[-1].start()
    for step in range(steps):
        sends[step].wait_recv()
        at = slice(step * chunk, (step + 1) * chunk)
        both = pf[:, at] + pr[:, at].astype(F32)
        for k in range(chunk // LANES):
            qf[pl.ds(step * (chunk // LANES) + k, half, stride=pitch), :] = both[
                :, k * LANES : (k + 1) * LANES
            ]

    out_copies = []
    for number, offset in list(enumerate(c_offsets))[::-1]:
        for loc in range(locals_):
            row = offset + loc
            qs[number, loc] = qf[row * pitch : row * pitch + pieces, :].astype(BF16)
        copy = pltpu.make_async_remote_copy(
            src_ref=qs.at[number],
            dst_ref=r2.at[number],
            send_sem=q_send.at[number],
            recv_sem=q_recv.at[number],
            device_id=peer(offset),
            device_id_type=pl.DeviceIdType.MESH,
        )
        copy.start()
        out_copies.append(copy)
    for copy in out_copies:
        copy.wait_recv()
    z_copies = []
    for loc in list(range(locals_))[::-1]:
        total = qf[loc * pitch : loc * pitch + pieces, :]
        for number in range(chips - 1):
            total += r2[number, loc].astype(F32)
        if loc == 0:
            of[...] = total
        else:
            ss[loc - 1] = total.astype(BF16)
            copy = pltpu.make_async_remote_copy(
                src_ref=ss.at[loc - 1],
                dst_ref=r3.at[loc - 1],
                send_sem=s_send.at[loc - 1],
                recv_sem=s_recv.at[loc - 1],
                device_id=peer(loc),
                device_id_type=pl.DeviceIdType.MESH,
            )
            copy.start()
            z_copies.append(copy)
    total = of[...]
    for copy in z_copies:
        copy.wait_recv()
    for loc in range(1, locals_):
        total += r3[loc - 1].astype(F32)
    out_ref[...] = total.astype(BF16)
    for copy in waits + sends + out_copies + z_copies:
        copy.wait_send()


def fused(nodes, locals_, tokens, w_gate, w_up, w_down, expert_ids, gate_ints):
    width = tokens.shape[1]
    experts, ffl = w_gate.shape[0], w_gate.shape[1]
    chips = nodes // 2
    rows = nodes * locals_
    half = rows // 2
    pieces = width // LANES
    pitch = -(-(pieces + 2) // 16) * 16
    steps = width // 1024 if width % 1024 == 0 else 1
    vmem = pl.BlockSpec(memory_space=pltpu.VMEM)
    hbm = pl.BlockSpec(memory_space=pl.ANY)
    dma = pltpu.SemaphoreType.DMA
    out = pl.pallas_call(
        functools.partial(kernel, nodes, locals_),
        out_shape=jax.ShapeDtypeStruct((pieces, LANES), BF16),
        in_specs=[vmem] * 3 + [hbm] * 3,
        out_specs=vmem,
        scratch_shapes=[
            pltpu.VMEM((experts, ffl, width), BF16),
            pltpu.VMEM((experts, ffl, width), BF16),
            pltpu.VMEM((experts, ffl, width), BF16),
            pltpu.VMEM((rows, pitch, LANES), BF16),
            pltpu.VMEM((rows * pitch, LANES), F32),
            pltpu.VMEM((rows, width), BF16),
            pltpu.VMEM((2, experts, ffl, rows), F32),
            pltpu.VMEM((half, width), BF16),
            pltpu.VMEM((half, width), BF16),
            pltpu.VMEM((half, width), F32),
            pltpu.VMEM((half * pitch, LANES), F32),
            pltpu.VMEM((chips - 1, locals_, pieces, LANES), BF16),
            pltpu.VMEM((chips - 1, locals_, pieces, LANES), BF16),
            pltpu.VMEM((locals_ - 1, pieces, LANES), BF16),
            pltpu.VMEM((locals_ - 1, pieces, LANES), BF16),
            pltpu.VMEM((pieces, LANES), F32),
            dma((3, experts)),
            dma((chips + locals_, rows)),
            dma((rows,)),
            dma((steps,)),
            dma((steps,)),
            dma((chips - 1,)),
            dma((chips - 1,)),
            dma((locals_ - 1,)),
            dma((locals_ - 1,)),
        ],
        compiler_params=pltpu.CompilerParams(
            collective_id=0, has_side_effects=True, vmem_limit_bytes=56 * 1024 * 1024
        ),
    )(tokens, expert_ids, gate_ints, w_gate, w_up, w_down)
    return out.reshape(1, width)


def route(nodes, locals_, tokens, w_gate, w_up, w_down, expert_ids, gate_ints):
    width = tokens.shape[1]
    power = (nodes & (nodes - 1)) == 0 and (locals_ & (locals_ - 1)) == 0
    small = (
        nodes * tokens.shape[0] <= CAP
        and tokens.shape[0] == 1
        and nodes >= 4
        and locals_ >= 2
        and nodes * w_gate.shape[0] <= 256
        and (nodes * locals_) % 32 == 0
        and width % LANES == 0
        and 3 * w_gate.size * 2 <= 32 * 1024 * 1024
    )
    if power and small:
        return fused(nodes, locals_, tokens, w_gate, w_up, w_down, expert_ids, gate_ints)
    return on_device(tokens, w_gate, w_up, w_down, expert_ids, gate_ints)


def solution(mesh):
    return jax.shard_map(
        functools.partial(route, mesh.shape["node"], mesh.shape["local"]),
        mesh=mesh,
        in_specs=(
            P(("node", "local"), None),
            P("node", "local", None),
            P("node", "local", None),
            P("node", "local", None),
            P(("node", "local"), None),
            P(("node", "local"), None),
        ),
        out_specs=P(("node", "local"), None),
        check_vma=False,
    )
```

```python
import functools

import jax
import jax.numpy as jnp
from jax import lax
from jax.experimental import pallas as pl
from jax.experimental.pallas import tpu as pltpu
from jax.sharding import PartitionSpec as P

CAP = 8


def on_device(tokens, w_gate, w_up, w_down, expert_ids, gate_ints):
    node_count = lax.axis_size("node")
    tok_dev = tokens.shape[0]
    model_width = tokens.shape[1]
    exp_node = w_gate.shape[0]
    slot_count = node_count * tok_dev
    wanted = jnp.arange(node_count * exp_node, dtype=jnp.int32).reshape(node_count, exp_node)
    matched = expert_ids[None, :, :, None] == wanted[:, None, None, :]
    gate_sums = jnp.sum(jnp.where(matched, gate_ints[None, :, :, None], 0), axis=2)
    is_hit = jnp.sum(gate_sums, axis=-1) > 0
    outgoing = jnp.where(is_hit[:, :, None], tokens[None, :, :], jnp.zeros_like(tokens)[None, :, :])
    rows_in, gates_in = (
        lax.all_to_all(outgoing, "node", split_axis=0, concat_axis=0, tiled=True),
        lax.all_to_all(
            gate_sums.astype(jnp.bfloat16), "node", split_axis=0, concat_axis=0, tiled=True
        ),
    )
    flat_rows = rows_in.reshape(slot_count, model_width)
    flat_gates = gates_in.reshape(slot_count, exp_node)
    present = (jnp.sum(flat_gates.astype(jnp.float32), axis=-1) > 0).astype(jnp.int32)
    slot_rank = jnp.cumsum(present) - present
    picker = (
        (present[None, :] > 0) & (slot_rank[None, :] == jnp.arange(CAP, dtype=jnp.int32)[:, None])
    ).astype(jnp.bfloat16)
    packed = jnp.dot(picker, flat_rows, preferred_element_type=jnp.float32).astype(jnp.bfloat16)
    packed_gates = jnp.dot(picker, flat_gates, preferred_element_type=jnp.float32).astype(
        jnp.bfloat16
    )
    all_rows, all_gates = (
        lax.all_gather(packed, "local", axis=0, tiled=True),
        lax.all_gather(packed_gates, "local", axis=0, tiled=True),
    )
    gate_act = jnp.einsum("rd,efd->ref", all_rows, w_gate, preferred_element_type=jnp.float32)
    up_act = jnp.einsum("rd,efd->ref", all_rows, w_up, preferred_element_type=jnp.float32)
    scales = all_gates.astype(jnp.float32) / 8.0
    hidden = (jax.nn.silu(gate_act) * up_act * scales[:, :, None]).astype(jnp.bfloat16)
    hidden = hidden.reshape(hidden.shape[0], -1)
    down_flat = w_down.reshape(-1, model_width)
    partial_value = jnp.dot(hidden, down_flat, preferred_element_type=jnp.float32)
    summed = lax.psum_scatter(
        partial_value.astype(jnp.bfloat16), "local", scatter_dimension=0, tiled=True
    )
    unpacked = jnp.dot(picker.T, summed, preferred_element_type=jnp.float32).astype(jnp.bfloat16)
    unpacked = unpacked.reshape(node_count, tok_dev, model_width)
    returned = lax.all_to_all(unpacked, "node", split_axis=0, concat_axis=0, tiled=True)
    return jnp.sum(returned.astype(jnp.float32), axis=0).astype(jnp.bfloat16)


LANES = 128
BF16 = jnp.bfloat16
F32 = jnp.float32


def flip(value, mask):
    bit = 1
    out = value
    while bit <= mask:
        if mask & bit:
            out = out + bit - 2 * bit * ((value // bit) % 2)
        bit *= 2
    return out


def kernel(
    nodes, locals_, tok_hbm, ids_hbm, gate_ints_hbm, wg_hbm, wu_hbm, wd_hbm, out_ref,
    tok_ref, ids_ref, gate_ints_ref, in_sem, wgu, wd, xbuf, xf, xs, acc, ps, pr, pf, qf, qs, r2, ss, r3, of,
    w_sem, x_send, x_recv, p_send, p_recv, q_send, q_recv, s_send, s_recv,
):
    chips = nodes // 2
    rows = nodes * locals_
    half = rows // 2
    width = tok_hbm.shape[1]
    chunk = 1024 if width % 1024 == 0 else width
    deep = 1792 if width % 1792 == 0 else chunk
    pieces = width // LANES
    pitch = xbuf.shape[1]
    experts, ffl = wg_hbm.shape[0], wg_hbm.shape[1]
    me_n = lax.axis_index("node")
    me_l = lax.axis_index("local")

    def peer(offset):
        core, rest = offset // half, offset % half
        chip, loc = rest // locals_, rest % locals_
        return (flip(me_n, chip * 2 + core), flip(me_l, loc))

    z_offsets = list(range(1, locals_))
    c_offsets = [c * locals_ for c in range(1, chips)]
    partner = half
    barrier = pltpu.get_barrier_semaphore()
    greeted = z_offsets + c_offsets + [partner]
    for offset in greeted:
        pl.semaphore_signal(
            barrier, inc=1, device_id=peer(offset), device_id_type=pl.DeviceIdType.MESH
        )

    small = []
    for which, (source, dest) in enumerate(
        ((tok_hbm, tok_ref), (ids_hbm, ids_ref), (gate_ints_hbm, gate_ints_ref))
    ):
        copy = pltpu.make_async_copy(source, dest, in_sem.at[which])
        copy.start()
        small.append(copy)
    xf[0:pitch, :] = jnp.zeros((pitch, LANES), F32)
    for copy in small:
        copy.wait()
    for k in range(pieces):
        xf[k : k + 1, :] = tok_ref[:, k * LANES : (k + 1) * LANES].astype(F32)
    top = ids_ref.shape[1]
    xf[pieces : pieces + 1, 0:top] = ids_ref[...].astype(F32)
    xf[pieces + 1 : pieces + 2, 0:top] = gate_ints_ref[...].astype(F32)
    xbuf[0] = xf[0:pitch, :].astype(BF16)

    pl.semaphore_wait(barrier, len(greeted))

    waits = []

    def block_copy(row, count, offset, slot):
        landing = row ^ offset if count == 1 else (row // locals_ * locals_ ^ offset) + row % locals_
        return pltpu.make_async_remote_copy(
            src_ref=xbuf.at[pl.ds(row, count)],
            dst_ref=xbuf.at[pl.ds(landing, count)],
            send_sem=x_send.at[slot, row],
            recv_sem=x_recv.at[landing],
            device_id=peer(offset),
            device_id_type=pl.DeviceIdType.MESH,
        )

    def send(row, count, offset, slot):
        copy = block_copy(row, count, offset, slot)
        copy.start()
        waits.append(copy)

    def arrive(row, count):
        pltpu.make_async_remote_copy(
            src_ref=xbuf.at[pl.ds(row, count)],
            dst_ref=xbuf.at[pl.ds(row, count)],
            send_sem=x_send.at[0, row],
            recv_sem=x_recv.at[row],
            device_id=peer(partner),
            device_id_type=pl.DeviceIdType.MESH,
        ).wait_recv()

    def widen(row):
        xf[row * pitch : (row + 1) * pitch, :] = xbuf[row].astype(F32)

    for number, offset in list(enumerate(z_offsets))[::-1]:
        send(0, 1, offset, 1 + chips + number)
    for number, offset in enumerate(c_offsets):
        send(0, 1, offset, 1 + number)
    send(0, 1, partner, 0)
    loads = []
    places = ((wg_hbm, wgu, 0), (wu_hbm, wgu, experts), (wd_hbm, wd, 0))
    for which, (source, dest, first) in enumerate(places):
        for e in range(experts):
            copy = pltpu.make_async_copy(
                source.at[e], dest.at[pl.ds((first + e) * ffl, ffl)], w_sem.at[which, e]
            )
            copy.start()
            loads.append(copy)

    for row in z_offsets:
        arrive(row, 1)
        for number, offset in enumerate(c_offsets):
            send(row, 1, offset, 1 + number)
        send(row, 1, partner, 0)
        widen(row)
    for loc in range(locals_):
        for offset in c_offsets:
            row = offset + loc
            arrive(row, 1)
            send(row, 1, partner, 0)
            widen(row)
    for row in range(half, rows):
        arrive(row, 1)
        widen(row)

    for k in range(pieces):
        xs[:, k * LANES : (k + 1) * LANES] = xf[pl.ds(k, rows, stride=pitch), :].astype(BF16)
    ids = xf[pl.ds(pieces, rows, stride=pitch), :]
    gates = xf[pl.ds(pieces + 1, rows, stride=pitch), :]
    scales = []
    for e in range(experts):
        named = (me_n * experts + e).astype(F32)
        picked = jnp.where(ids == named, gates, 0.0)
        scales.append(jnp.sum(picked, axis=1, keepdims=True) / 8.0)

    for copy in loads[: 2 * experts]:
        copy.wait()
    acc[...] = jnp.zeros_like(acc)

    def depth_step(step, carry):
        at = pl.ds(pl.multiple_of(step * deep, deep), deep)
        acc[...] += lax.dot_general(
            wgu[:, at], xs[:, at], (((1,), (1,)), ((), ())), preferred_element_type=F32
        )
        return carry

    lax.fori_loop(0, width // deep, depth_step, 0)
    hidden = []
    for e in range(experts):
        g = acc[e * ffl : (e + 1) * ffl, :].T
        u = acc[(experts + e) * ffl : (experts + e + 1) * ffl, :].T
        hidden.append((g / (1.0 + jnp.exp(-g)) * u * scales[e]).astype(BF16))
    hidden = jnp.concatenate(hidden, axis=1)

    for copy in loads[2 * experts :]:
        copy.wait()
    sends = []
    steps = width // chunk

    def partner_copy(step):
        at = pl.ds(step * chunk, chunk)
        return pltpu.make_async_remote_copy(
            src_ref=ps.at[:, at],
            dst_ref=pr.at[:, at],
            send_sem=p_send.at[step],
            recv_sem=p_recv.at[step],
            device_id=peer(partner),
            device_id_type=pl.DeviceIdType.MESH,
        )

    per = chunk // LANES
    first_group = (steps + 1) // 2
    groups = [(0, first_group), (first_group, steps)]
    groups = [(low, high) for low, high in groups if high > low]
    out_copies = []
    z_copies = []

    def combine(step):
        sends[step].wait_recv()
        at = slice(step * chunk, (step + 1) * chunk)
        both = pf[:, at] + pr[:, at].astype(F32)
        for k in range(per):
            qf[pl.ds(step * per + k, half, stride=pitch), :] = both[
                :, k * LANES : (k + 1) * LANES
            ]

    def send_chips(group):
        low, high = groups[group][0] * per, groups[group][1] * per
        for number, offset in list(enumerate(c_offsets))[::-1]:
            for loc in range(locals_):
                at = (offset + loc) * pitch
                qs[group, number, loc, 0 : high - low] = qf[at + low : at + high, :].astype(BF16)
            copy = pltpu.make_async_remote_copy(
                src_ref=qs.at[group, number, :, pl.ds(0, high - low)],
                dst_ref=r2.at[group, number, :, pl.ds(0, high - low)],
                send_sem=q_send.at[group, number],
                recv_sem=q_recv.at[group, number],
                device_id=peer(offset),
                device_id_type=pl.DeviceIdType.MESH,
            )
            copy.start()
            out_copies.append(copy)

    lag = 7
    for step in range(steps + lag):
        if step < steps:
            at = slice(step * chunk, (step + 1) * chunk)
            part = jnp.dot(hidden, wd[:, at], preferred_element_type=F32)
            ps[:, at] = part[half:].astype(BF16)
            pf[:, at] = part[:half]
            sends.append(partner_copy(step))
        if 1 <= step <= steps:
            sends[step - 1].start()
        if step >= lag:
            combine(step - lag)
            for group, (low, high) in enumerate(groups):
                if step - lag == high - 1:
                    send_chips(group)

    for group, (first, last) in enumerate(groups):
        low, high = first * per, last * per
        for copy in out_copies[group * (chips - 1) : (group + 1) * (chips - 1)]:
            copy.wait_recv()
        for loc in list(range(locals_))[::-1]:
            total = qf[loc * pitch + low : loc * pitch + high, :]
            for number in range(chips - 1):
                total += r2[group, number, loc, 0 : high - low].astype(F32)
            if loc == 0:
                of[low:high, :] = total
            else:
                ss[group, loc - 1, 0 : high - low] = total.astype(BF16)
                copy = pltpu.make_async_remote_copy(
                    src_ref=ss.at[group, loc - 1, pl.ds(0, high - low)],
                    dst_ref=r3.at[group, loc - 1, pl.ds(0, high - low)],
                    send_sem=s_send.at[group, loc - 1],
                    recv_sem=s_recv.at[group, loc - 1],
                    device_id=peer(loc),
                    device_id_type=pl.DeviceIdType.MESH,
                )
                copy.start()
                z_copies.append(copy)
    for group, (first, last) in enumerate(groups):
        low, high = first * per, last * per
        total = of[low:high, :]
        for copy in z_copies[group * (locals_ - 1) : (group + 1) * (locals_ - 1)]:
            copy.wait_recv()
        for loc in range(1, locals_):
            total += r3[group, loc - 1, 0 : high - low].astype(F32)
        for k in range(high - low):
            out_ref[:, (low + k) * LANES : (low + k + 1) * LANES] = total[k : k + 1, :].astype(BF16)
    for copy in waits + sends + out_copies + z_copies:
        copy.wait_send()


def fused(nodes, locals_, tokens, w_gate, w_up, w_down, expert_ids, gate_ints):
    width = tokens.shape[1]
    experts, ffl = w_gate.shape[0], w_gate.shape[1]
    chips = nodes // 2
    rows = nodes * locals_
    half = rows // 2
    pieces = width // LANES
    pitch = -(-(pieces + 2) // 16) * 16
    steps = width // 1024 if width % 1024 == 0 else 1
    most = (steps + 1) // 2 * (width // steps // LANES)
    vmem = pl.BlockSpec(memory_space=pltpu.VMEM)
    hbm = pl.BlockSpec(memory_space=pl.ANY)
    dma = pltpu.SemaphoreType.DMA
    return pl.pallas_call(
        functools.partial(kernel, nodes, locals_),
        out_shape=jax.ShapeDtypeStruct((1, width), BF16),
        in_specs=[hbm] * 6,
        out_specs=vmem,
        scratch_shapes=[
            pltpu.VMEM(tokens.shape, BF16),
            pltpu.VMEM(expert_ids.shape, jnp.int32),
            pltpu.VMEM(gate_ints.shape, jnp.int32),
            dma((3,)),
            pltpu.VMEM((2 * experts * ffl, width), BF16),
            pltpu.VMEM((experts * ffl, width), BF16),
            pltpu.VMEM((rows, pitch, LANES), BF16),
            pltpu.VMEM((rows * pitch, LANES), F32),
            pltpu.VMEM((rows, width), BF16),
            pltpu.VMEM((2 * experts * ffl, rows), F32),
            pltpu.VMEM((half, width), BF16),
            pltpu.VMEM((half, width), BF16),
            pltpu.VMEM((half, width), F32),
            pltpu.VMEM((half * pitch, LANES), F32),
            pltpu.VMEM((2, chips - 1, locals_, most, LANES), BF16),
            pltpu.VMEM((2, chips - 1, locals_, most, LANES), BF16),
            pltpu.VMEM((2, locals_ - 1, most, LANES), BF16),
            pltpu.VMEM((2, locals_ - 1, most, LANES), BF16),
            pltpu.VMEM((pieces, LANES), F32),
            dma((3, experts)),
            dma((chips + locals_, rows)),
            dma((rows,)),
            dma((steps,)),
            dma((steps,)),
            dma((2, chips - 1)),
            dma((2, chips - 1)),
            dma((2, locals_ - 1)),
            dma((2, locals_ - 1)),
        ],
        compiler_params=pltpu.CompilerParams(
            collective_id=0, has_side_effects=True, vmem_limit_bytes=56 * 1024 * 1024
        ),
    )(tokens, expert_ids, gate_ints, w_gate, w_up, w_down)


def route(nodes, locals_, tokens, w_gate, w_up, w_down, expert_ids, gate_ints):
    width = tokens.shape[1]
    power = (nodes & (nodes - 1)) == 0 and (locals_ & (locals_ - 1)) == 0
    small = (
        nodes * tokens.shape[0] <= CAP
        and tokens.shape[0] == 1
        and nodes >= 4
        and locals_ >= 2
        and nodes * w_gate.shape[0] <= 256
        and (nodes * locals_) % 32 == 0
        and width % LANES == 0
        and 3 * w_gate.size * 2 <= 32 * 1024 * 1024
    )
    if power and small:
        return fused(nodes, locals_, tokens, w_gate, w_up, w_down, expert_ids, gate_ints)
    return on_device(tokens, w_gate, w_up, w_down, expert_ids, gate_ints)


def solution(mesh):
    return jax.shard_map(
        functools.partial(route, mesh.shape["node"], mesh.shape["local"]),
        mesh=mesh,
        in_specs=(
            P(("node", "local"), None),
            P("node", "local", None),
            P("node", "local", None),
            P("node", "local", None),
            P(("node", "local"), None),
            P(("node", "local"), None),
        ),
        out_specs=P(("node", "local"), None),
        check_vma=False,
    )
```
